256 devices in a mesh: ga: 4 (over y, x), row: 32 (over z), col: 2 (over core).
Axes of the slice: x: 2, y: 2, z: 32, core: 2. Of those that a mesh axis runs over, the one named last changes fastest.
The devices are a block of a 4x8x32 slice.
Arguments:
- pair: bfloat16 [2048, 512, 128], P(('ga', 'row', 'col')), parts along dimension 0, may hold values from -480 to 480
- residue_mask: int32 [2048], P('ga'), parts along dimension 0, may hold values from 0 to 1, as said below
- targets: int32 [2048, 512], P(('ga', 'row', 'col')), parts along dimension 0, may hold values from 0 to 63
- ln_gain: float32 [2, 128], replicated, may hold values from 0.25 to 1.75
- ln_shift: float32 [2, 128], replicated, may hold values from -3 to 3
- w_in: bfloat16 [5, 128, 128], P(None, None, 'col'), may hold values from -0.5 to 0.5
- b_in: float32 [5, 128], replicated, may hold values from -3 to 3
- w_out: bfloat16 [128, 128], P('col'), may hold values from -0.5 to 0.5
- b_out: float32 [128], replicated, may hold values from -3 to 3
- head_weight: bfloat16 [128, 64], replicated, may hold values from -0.5 to 0.5
- head_bias: float32 [64], replicated, may hold values from -4 to 4
Outputs:
- update: bfloat16 [2048, 512, 128], P(('ga', 'row', 'col')), parts along dimension 0
- pair_loss: float32 [2048, 512], P(('ga', 'row', 'col')), parts along dimension 0
The draws below stay inside these ranges and needn't reach their ends.
There are 4 independent parts, one for each index of `ga`. The reference program is written for one: setup_inputs(seed, part) draws one part's arguments, and reference() takes and returns one part's arrays. A program takes and returns all parts, laid end to end along the dimension named above; an argument that names none is the same for every part. Nothing has to cross between parts.
Inputs may be any that keep to these rules, and one draw needn't show every extreme that they name: `residue_mask`: each part's entries are 1 for residues 0 to some length - 1 and 0 after it; the length is at least 256 and at most 512.
All inputs are finite; a program needn't handle non-finite values.
Results may differ from the reference program's by a relative error of at most 0.0055.
Values may be sent and summed in bfloat16 or wider, within the bound.
No kernel may reach another device: no remote copies, remote signals or barrier semaphores. Data moves between devices by JAX's collectives and lax.ppermute only.
A program may use at most 64 MiB of HBM per device.

```python
import jax
import jax.numpy as jnp
from jax import lax

D = 128
BINS = 64
RESIDUES = 512


def draw_pair(key, part):
    first_key, second_key = jax.random.split(key)
    values = jnp.clip(jax.random.normal(first_key, (RESIDUES, RESIDUES, D), jnp.float32), -6.0, 6.0)
    return values.astype(jnp.bfloat16)


def draw_residue_mask(key, part):
    crop_length = jax.random.randint(key, (), RESIDUES // 2, RESIDUES + 1)
    return (jnp.arange(RESIDUES) < crop_length).astype(jnp.int32)


def set_ends(result, key, smallest, largest):
    extent = result.shape
    spot = [jax.random.randint(jax.random.fold_in(key, axis), (), 0, extent[axis]) for axis in range(len(extent))]
    result = result.at[tuple(spot)].set(smallest)
    longest = extent.index(max(extent))
    spot[longest] = (spot[longest] + 1) % extent[longest]
    return result.at[tuple(spot)].set(largest)


def shard_levels(key, dims, pieces, least, high):
    gain, own = 1.0, jax.random.fold_in(key, 6)
    for dim, parts in pieces:
        steps = jnp.exp(jax.random.uniform(jax.random.fold_in(own, dim), (parts,), jnp.float32, least / len(pieces), high / len(pieces)))
        gain = gain * jnp.repeat(steps, dims[dim] // parts).reshape([-1 if axis == dim else 1 for axis in range(len(dims))])
    return gain


def gaussian(own_key, dims, scale, bound, cuts=(), kind=jnp.bfloat16):
    drawn = scale * jax.random.normal(own_key, dims, jnp.float32)
    if cuts:
        drawn = drawn * shard_levels(own_key, dims, cuts, -0.22, 0.18)
    return jnp.clip(drawn, -bound, bound).astype(kind)


def setup_inputs(seed: int = 0, part: int = 0) -> dict:
    key_list = jax.random.split(jax.random.key(seed), 12)
    part_keys = jax.random.split(jax.random.fold_in(key_list[11], part), 12)
    pair = draw_pair(jax.random.fold_in(jax.random.fold_in(key_list[11], part), 71), part)
    residue_mask = draw_residue_mask(jax.random.fold_in(jax.random.fold_in(key_list[11], part), 71), part)
    targets = set_ends(jax.random.randint(part_keys[2], (RESIDUES, RESIDUES), 0, BINS), jax.random.fold_in(part_keys[2], 1), 0, BINS - 1).astype(jnp.int32)
    ln_gain = jnp.clip(1.0 + 0.15 * jax.random.normal(key_list[3], (2, D), jnp.float32), 0.25, 1.75)
    ln_shift = gaussian(key_list[4], (2, D), 0.3, 3.0, (), jnp.float32)
    w_in = gaussian(key_list[5], (5, D, D), D ** -0.5, 0.5, ((2, 2),))
    b_in = gaussian(key_list[6], (5, D), 0.5, 3.0, (), jnp.float32)
    w_out = gaussian(key_list[7], (D, D), D ** -0.5, 0.5, ((0, 2),))
    b_out = gaussian(key_list[8], (D,), 0.5, 3.0, (), jnp.float32)
    head_weight = gaussian(key_list[9], (D, BINS), D ** -0.5, 0.5)
    head_bias = gaussian(key_list[10], (BINS,), 1.0, 4.0, (), jnp.float32)
    return dict(pair=pair, residue_mask=residue_mask, targets=targets, ln_gain=ln_gain, ln_shift=ln_shift, w_in=w_in, b_in=b_in, w_out=w_out, b_out=b_out, head_weight=head_weight, head_bias=head_bias)


def normalize(values, gain_vec, shift_vec, epsilon):
    average = lax.optimization_barrier(jnp.mean(values, axis=-1, keepdims=True))
    centred = values - average
    spread = lax.optimization_barrier(jnp.mean(centred * centred, axis=-1, keepdims=True))
    return centred * lax.rsqrt(spread + epsilon) * gain_vec + shift_vec

def reference(pair, residue_mask, targets, ln_gain, ln_shift, w_in, b_in, w_out, b_out, head_weight, head_bias):
    res_mask = residue_mask.astype(jnp.float32)
    row_block = 32
    block_count = RESIDUES // row_block
    pair_blocks = pair.reshape(block_count, row_block, RESIDUES, D)
    mask_blocks = res_mask.reshape(block_count, row_block)
    weights_in = w_in.astype(jnp.float32)

    def project(operands):
        rows_pair, rows_mask = operands
        normed = normalize(rows_pair.astype(jnp.float32), ln_gain[0], ln_shift[0], 0.1).astype(jnp.bfloat16)
        projected = jnp.einsum('ikc,ncd->nikd', normed.astype(jnp.float32), weights_in) + b_in[:, None, None, :]
        masks = rows_mask[:, None, None] * res_mask[None, :, None]
        left_side = (masks * jax.nn.sigmoid(projected[1]) * projected[0]).astype(jnp.bfloat16)
        right_side = (masks * jax.nn.sigmoid(projected[3]) * projected[2]).astype(jnp.bfloat16)
        gate_value = jax.nn.sigmoid(projected[4])
        return (left_side, right_side, gate_value)
    lefts, rights, gates = lax.map(project, (pair_blocks, mask_blocks))
    left_chan = jnp.transpose(lefts.reshape(RESIDUES, RESIDUES, D), (2, 0, 1))
    right_chan = jnp.transpose(rights.reshape(RESIDUES, RESIDUES, D), (2, 0, 1))

    def triangle(operands):
        left_part, right_part = operands
        product = jnp.einsum('cik,cjk->cij', left_part.astype(jnp.float32), right_part.astype(jnp.float32))
        return product.astype(jnp.bfloat16)
    outer_prod = lax.map(triangle, (left_chan.reshape(D // 8, 8, RESIDUES, RESIDUES), right_chan.reshape(D // 8, 8, RESIDUES, RESIDUES)))
    outer_rows = jnp.transpose(outer_prod.reshape(D, RESIDUES, RESIDUES), (1, 2, 0))
    weights_out = w_out.astype(jnp.float32)
    head_float = head_weight.astype(jnp.float32)

    def finish(operands):
        rows_outer, rows_gate, rows_pair = operands
        normed_outer = normalize(rows_outer.astype(jnp.float32), ln_gain[1], ln_shift[1], 1.0).astype(jnp.bfloat16)
        mixed = jnp.einsum('ijc,cd->ijd', normed_outer.astype(jnp.float32), weights_out) + b_out
        update = (rows_gate * mixed).astype(jnp.bfloat16)
        new_pair = (rows_pair.astype(jnp.float32) + update.astype(jnp.float32)).astype(jnp.bfloat16)
        logits = jnp.einsum('ijc,cb->ijb', new_pair.astype(jnp.float32), head_float) + head_bias
        return (update, logits)
    updates, logit_blocks = lax.map(finish, (outer_rows.reshape(block_count, row_block, RESIDUES, D), gates, pair_blocks))
    update = updates.reshape(RESIDUES, RESIDUES, D)
    logits = logit_blocks.reshape(RESIDUES, RESIDUES, BINS)
    symmetric = logits + jnp.transpose(logits, (1, 0, 2))
    log_total = jax.nn.logsumexp(symmetric, axis=-1)
    picked = jnp.take_along_axis(symmetric, targets[..., None].astype(jnp.int32), axis=-1)[..., 0]
    pair_loss = res_mask[:, None] * res_mask[None, :] * (log_total - picked)
    return (update, pair_loss)
```

```python
import functools

import jax
import jax.numpy as jnp
from jax import lax
from jax.experimental import pallas as pl
from jax.experimental.pallas import tpu as pltpu
from jax.sharding import PartitionSpec as P

F32 = jnp.float32
BF16 = jnp.bfloat16
NT = (((1,), (1,)), ((), ()))
TN = (((0,), (0,)), ((), ()))


def dot(a, b, dims):
    return lax.dot_general(a, b, dims, preferred_element_type=F32)


def input_norm(pair_ref, gain_ref, shift_ref):
    x = pair_ref[...].astype(F32)
    x = x.reshape(-1, x.shape[-1])
    centred = x - jnp.mean(x, axis=-1, keepdims=True)
    spread = jnp.mean(centred * centred, axis=-1, keepdims=True)
    normed = centred * lax.rsqrt(spread + 0.1) * gain_ref[0:1] + shift_ref[0:1]
    return normed.astype(BF16)


def sides_kernel(mask_sref, pair_ref, maskk_ref, w_ref, b_ref, gain_ref, shift_ref, out_ref, stage):
    rows, width, chans = pair_ref.shape
    share = out_ref.shape[1] // 2
    chips = out_ref.shape[0]
    base = (lax.axis_index("row") * lax.axis_size("col") + lax.axis_index("col")) * rows
    normed = input_norm(pair_ref, gain_ref, shift_ref)
    bias = jnp.transpose(jnp.concatenate([b_ref[...], jnp.zeros((3, chans), F32)], axis=0))
    mask_k = maskk_ref[...].astype(F32)
    for side in range(2):
        value = dot(w_ref[2 * side], normed, NT) + bias[:, 2 * side : 2 * side + 1]
        gate = dot(w_ref[2 * side + 1], normed, NT) + bias[:, 2 * side + 1 : 2 * side + 2]
        value = jax.nn.sigmoid(gate) * value
        for r in range(rows):
            mask = mask_k * mask_sref[base + r].astype(F32)
            part = value[:, r * width : (r + 1) * width] * mask
            for c in range(share):
                stage[pl.ds((side * share + c) * rows + r, chips, stride=2 * share * rows), :] = part[
                    c * chips : (c + 1) * chips
                ]
    out_ref[...] = stage[...].reshape(out_ref.shape).astype(BF16)


def make_sides(pair, mask, w_t, b_in, gain, shift, chips):
    rows, length, chans = pair.shape
    share = chans // chips
    width = 128
    whole = lambda *shape: pl.BlockSpec(shape, lambda k: (0,) * len(shape))
    return pl.pallas_call(
        sides_kernel,
        grid=(length // width,),
        in_specs=[
            pl.BlockSpec(memory_space=pltpu.SMEM),
            pl.BlockSpec((rows, width, chans), lambda k: (0, k, 0)),
            pl.BlockSpec((1, width), lambda k: (0, k)),
            whole(*w_t.shape),
            whole(*b_in.shape),
            whole(*gain.shape),
            whole(*shift.shape),
        ],
        out_specs=pl.BlockSpec((chips, 2 * share, rows, width), lambda k: (0, 0, 0, k)),
        out_shape=jax.ShapeDtypeStruct((chips, 2 * share, rows, length), BF16),
        scratch_shapes=[pltpu.VMEM((chips * 2 * share * rows, width), F32)],
        name="sides",
    )(mask, pair, mask.reshape(1, length), w_t, b_in, gain, shift)


def gate_kernel(pair_ref, w_ref, b_ref, gain_ref, shift_ref, out_ref):
    normed = input_norm(pair_ref, gain_ref, shift_ref)
    pre = dot(normed, w_ref[4], NT) + b_ref[4:5]
    out_ref[...] = jax.nn.sigmoid(pre).reshape(out_ref.shape)


def make_gate(pair, w_t, b_in, gain, shift):
    rows, length, chans = pair.shape
    whole = lambda *shape: pl.BlockSpec(shape, lambda r: (0,) * len(shape))
    return pl.pallas_call(
        gate_kernel,
        grid=(rows // 2,),
        in_specs=[
            pl.BlockSpec((2, length, chans), lambda r: (r, 0, 0)),
            whole(*w_t.shape),
            whole(*b_in.shape),
            whole(*gain.shape),
            whole(*shift.shape),
        ],
        out_specs=pl.BlockSpec((2, length, chans), lambda r: (r, 0, 0)),
        out_shape=jax.ShapeDtypeStruct((rows, length, chans), F32),
        cost_estimate=pl.CostEstimate(
            flops=2 * rows * length * chans * chans, bytes_accessed=rows * length * chans * 6, transcendentals=0
        ),
        name="gate",
    )(pair, w_t, b_in, gain, shift)


def triangle_kernel(left_ref, right_ref, other_ref, out_ref):
    chips, _, rows, length = left_ref.shape
    half = chips * rows
    left = left_ref[...].reshape(half, length)
    own = dot(left, right_ref[...].reshape(half, length), NT).astype(BF16)
    other = dot(left, other_ref[...].reshape(half, length), NT).astype(BF16)
    core = lax.axis_index("col")

    def put(first, second):
        out_ref[:, :, :, 0:half] = first.reshape(chips, 1, rows, half)
        out_ref[:, :, :, half : 2 * half] = second.reshape(chips, 1, rows, half)

    pl.when(core == 0)(lambda: put(own, other))
    pl.when(core != 0)(lambda: put(other, own))


def make_triangle(sides, other):
    chips, double, rows, length = sides.shape
    share = double // 2
    block = (chips, 1, rows, length)
    return pl.pallas_call(
        triangle_kernel,
        grid=(share,),
        in_specs=[
            pl.BlockSpec(block, lambda c: (0, c, 0, 0)),
            pl.BlockSpec(block, lambda c: (0, share + c, 0, 0)),
            pl.BlockSpec(block, lambda c: (0, c, 0, 0)),
        ],
        out_specs=pl.BlockSpec(block, lambda c: (0, c, 0, 0)),
        out_shape=jax.ShapeDtypeStruct((chips, share, rows, 2 * chips * rows), BF16),
        name="triangle",
    )(sides, sides, other)


def finish_kernel(
    prod_ref,
    gate_ref,
    pair_ref,
    w_ref,
    b_ref,
    cols_ref,
    headw_ref,
    headb_ref,
    headbt_ref,
    update_ref,
    send_ref,
    own_ref,
    stage,
    sendst,
):
    chans, rows, width = prod_ref.shape
    bins = headw_ref.shape[1]
    core = pl.program_id(1)
    x = prod_ref[...].astype(F32)
    centred = x - jnp.mean(x, axis=0, keepdims=True)
    spread = jnp.mean(centred * centred, axis=0, keepdims=True)
    stage[...] = (centred * lax.rsqrt(spread + 1.0)).reshape(chans * rows, width)
    gain, shift = cols_ref[:, 0:1], cols_ref[:, 1:2]
    b_out = b_ref[...]
    head_w = headw_ref[...]
    head_two = jnp.concatenate([head_w, head_w], axis=1)
    lane = lax.broadcasted_iota(jnp.int32, (width, 2 * bins), 1)
    mine = (lane >= bins) == (core == 1)
    for r in range(rows):
        normed = (stage[pl.ds(r, chans, stride=rows), :] * gain + shift).astype(BF16)
        mixed = dot(normed, w_ref[...], TN) + b_out
        gate = gate_ref[r].reshape(width, chans)
        update = (gate * mixed).astype(BF16)
        update_ref[r] = update.reshape(update_ref.shape[1:])
        pair = pair_ref[r].reshape(width, chans)
        new_pair = (pair.astype(F32) + update.astype(F32)).astype(BF16)
        own_ref[pl.ds(r, bins, stride=rows), :] = dot(head_w, new_pair, (((0,), (1,)), ((), ()))) + headbt_ref[...]
        logits = dot(new_pair, head_two, (((1,), (0,)), ((), ()))) + headb_ref[...]
        at = pl.ds(r, width, stride=rows)

        @pl.when(core == 0)
        def _():
            sendst[at, :] = logits

        @pl.when(core == 1)
        def _():
            sendst[at, :] = jnp.where(mine, logits, sendst[at, :])

    @pl.when(core == 1)
    def _():
        send_ref[...] = sendst[...].reshape(send_ref.shape).astype(BF16)


def make_finish(prod, gate, pair, w_out, b_out, cols, head_w, head_b):
    chips = prod.shape[0]
    rows, length, chans = pair.shape
    bins = head_w.shape[1]
    cores = 2
    width = 128
    steps = length // (cores * width)
    near = chips // steps
    prod = prod.reshape(chans, rows, length)
    view = (rows, chips, cores, rows, chans)
    block = (rows, near, 1, rows, chans)
    at = lambda z, t: (0, z, t, 0, 0)
    whole = lambda *shape: pl.BlockSpec(shape, lambda z, t: (0,) * len(shape))
    head_row = jnp.concatenate([head_b, head_b]).reshape(1, 2 * bins)
    update, send, own = pl.pallas_call(
        finish_kernel,
        grid=(steps, cores),
        in_specs=[
            pl.BlockSpec((chans, rows, width), lambda z, t: (0, 0, t * steps + z)),
            pl.BlockSpec(block, at),
            pl.BlockSpec(block, at),
            whole(*w_out.shape),
            whole(1, chans),
            whole(*cols.shape),
            whole(*head_w.shape),
            whole(1, 2 * bins),
            whole(bins, 1),
        ],
        out_specs=[
            pl.BlockSpec(block, at),
            pl.BlockSpec((near, rows, rows, 2 * bins), lambda z, t: (z, 0, 0, 0)),
            pl.BlockSpec((bins * rows, width), lambda z, t: (0, t * steps + z)),
        ],
        out_shape=[
            jax.ShapeDtypeStruct(view, BF16),
            jax.ShapeDtypeStruct((chips, rows, rows, 2 * bins), BF16),
            jax.ShapeDtypeStruct((bins * rows, length), F32),
        ],
        scratch_shapes=[
            pltpu.VMEM((chans * rows, width), F32),
            pltpu.VMEM((near * rows * rows, 2 * bins), F32),
        ],
        name="finish",
    )(
        prod,
        gate.reshape(view),
        pair.reshape(view),
        w_out,
        b_out.reshape(1, chans),
        cols,
        head_w,
        head_row,
        head_b.reshape(bins, 1),
    )
    return update.reshape(rows, length, chans), send, own


def loss_kernel(mask_sref, own_ref, mine_ref, other_ref, targets_ref, maskk_ref, out_ref, stage):
    chips, rows, _, lanes = mine_ref.shape
    bins = lanes // 2
    half = chips * rows
    length = 2 * half
    core = lax.axis_index("col")
    base = (lax.axis_index("row") * lax.axis_size("col") + core) * rows
    pick_row = lax.broadcasted_iota(jnp.int32, (bins, lanes), 0) + core * bins
    pick = jnp.where(pick_row == lax.broadcasted_iota(jnp.int32, (bins, lanes), 1), 1.0, 0.0).astype(BF16)
    for r in range(rows):
        at = pl.ds(r, bins, stride=rows)
        mine = dot(pick, mine_ref[:, r].reshape(half, lanes), NT)
        other = dot(pick, other_ref[:, r].reshape(half, lanes), NT)
        first = jnp.where(core == 0, mine, other)
        second = jnp.where(core == 0, other, mine)
        for q in range(half // 128):
            stage[q, at, :] = first[:, q * 128 : (q + 1) * 128]
            stage[half // 128 + q, at, :] = second[:, q * 128 : (q + 1) * 128]
    mirrored = jnp.concatenate([stage[q] for q in range(length // 128)], axis=1)
    symmetric = (own_ref[...] + mirrored).reshape(bins, rows, length)
    top = jnp.max(symmetric, axis=0)
    total = jnp.sum(jnp.exp(symmetric - top[None]), axis=0)
    bin_index = lax.broadcasted_iota(jnp.int32, (bins, rows, length), 0)
    picked = jnp.sum(jnp.where(targets_ref[...][None] == bin_index, symmetric, 0.0), axis=0)
    loss = top + jnp.log(total) - picked
    high = loss.astype(BF16)
    rest = loss - high.astype(F32)
    middle = rest.astype(BF16)
    low = (rest - middle.astype(F32)).astype(BF16)
    spot = lax.broadcasted_iota(jnp.int32, (length, length), 0)
    place = lax.broadcasted_iota(jnp.int32, (length, length), 1)
    come = (place // rows % 2) * half + (place // (2 * rows)) * rows + place % rows
    order = jnp.where(spot == come, 1.0, 0.0).astype(BF16)
    natural = dot(high, order, (((1,), (0,)), ((), ())))
    natural += dot(middle, order, (((1,), (0,)), ((), ())))
    natural += dot(low, order, (((1,), (0,)), ((), ())))
    row = lax.broadcasted_iota(jnp.int32, (rows, length), 0)
    mask_i = jnp.zeros((rows, length), F32)
    for r in range(rows):
        mask_i = jnp.where(row == r, mask_sref[base + r].astype(F32), mask_i)
    out_ref[...] = mask_i * maskk_ref[...].astype(F32) * natural


def make_loss(mask, own, mine, other, targets):
    rows, length = targets.shape
    whole = lambda *shape: pl.BlockSpec(shape, lambda: (0,) * len(shape))
    return pl.pallas_call(
        loss_kernel,
        in_specs=[
            pl.BlockSpec(memory_space=pltpu.SMEM),
            whole(*own.shape),
            whole(*mine.shape),
            whole(*other.shape),
            whole(*targets.shape),
            whole(1, length),
        ],
        out_specs=whole(rows, length),
        out_shape=jax.ShapeDtypeStruct((rows, length), F32),
        scratch_shapes=[pltpu.VMEM((length // 128, own.shape[0], 128), F32)],
        name="loss",
    )(mask, own, mine, other, targets, mask.reshape(1, length))


def local(
    pair, residue_mask, targets, ln_gain, ln_shift, w_in, b_in, w_out, b_out, head_weight, head_bias
):
    rows, length, chans = pair.shape
    chips = lax.axis_size("row")
    share = chans // chips
    swap = functools.partial(lax.ppermute, axis_name="col", perm=[(0, 1), (1, 0)])
    exchange = lambda v: lax.all_to_all(v, "row", split_axis=0, concat_axis=0, tiled=True)
    w_t = lax.all_gather(jnp.transpose(w_in, (0, 2, 1)), "col", axis=1, tiled=True)
    sides = make_sides(pair, residue_mask, w_t, b_in, ln_gain, ln_shift, chips)
    sides = exchange(sides)
    gate = make_gate(pair, w_t, b_in, ln_gain, ln_shift)
    by_owner = lambda v: jnp.swapaxes(v.reshape(share, chips, -1), 0, 1).reshape(chans, -1)
    w_full = by_owner(lax.all_gather(w_out, "col", axis=0, tiled=True))
    cols = by_owner(jnp.stack([ln_gain[1], ln_shift[1]], axis=1))
    targets = jnp.swapaxes(targets.reshape(rows, chips, 2, rows), 1, 2).reshape(rows, length)
    product = make_triangle(sides, swap(sides[:, share:]))
    product = exchange(product)
    update, send, own = make_finish(product, gate, pair, w_full, b_out, cols, head_weight, head_bias)
    mine = exchange(send)
    loss = make_loss(residue_mask, own, mine, swap(mine), targets)
    return (update, loss)


def solution(mesh):
    placed = (
        P(("ga", "row", "col"), None, None),
        P("ga"),
        P(("ga", "row", "col"), None),
        P(),
        P(),
        P(None, None, "col"),
        P(),
        P("col", None),
        P(),
        P(),
        P(),
    )
    return jax.shard_map(
        local,
        mesh=mesh,
        in_specs=placed,
        out_specs=(P(("ga", "row", "col"), None, None), P(("ga", "row", "col"), None)),
        check_vma=False,
    )
```

```python
import functools

import jax
import jax.numpy as jnp
from jax import lax
from jax.experimental import pallas as pl
from jax.experimental.pallas import tpu as pltpu
from jax.sharding import PartitionSpec as P

F32 = jnp.float32
BF16 = jnp.bfloat16
NT = (((1,), (1,)), ((), ()))
TN = (((0,), (0,)), ((), ()))


def dot(a, b, dims):
    return lax.dot_general(a, b, dims, preferred_element_type=F32)


def whole(*shape):
    return pl.BlockSpec(shape, lambda *_: (0,) * len(shape))


def in_vmem():
    return pl.BlockSpec(memory_space=pltpu.VMEM)


def pinned(*arrays):
    return [pltpu.with_memory_space_constraint(a, pltpu.VMEM) for a in arrays]


def norm_kernel(pair_ref, gain_ref, shift_ref, out_ref):
    chans = pair_ref.shape[-1]
    pair = pair_ref[...].reshape(-1, chans)
    centred = pair.astype(F32) - dot(pair, jnp.full((chans, chans), 1.0 / chans, BF16), NT)
    spread = jnp.mean(centred * centred, axis=-1, keepdims=True)
    normed = centred * lax.rsqrt(spread + 0.1) * gain_ref[0:1] + shift_ref[0:1]
    rows = pair_ref.shape[0]
    out_ref[pl.ds(pl.program_id(0) * rows, rows)] = normed.astype(BF16).reshape(pair_ref.shape)


def make_norm(pair, gain, shift):
    rows, length, chans = pair.shape
    return pl.pallas_call(
        norm_kernel,
        grid=(rows // 2,),
        in_specs=[
            pl.BlockSpec((2, length, chans), lambda r: (r, 0, 0)),
            whole(*gain.shape),
            whole(*shift.shape),
        ],
        out_specs=in_vmem(),
        out_shape=jax.ShapeDtypeStruct(pair.shape, BF16),
        cost_estimate=pl.CostEstimate(
            flops=rows * length * chans * 100, bytes_accessed=rows * length * chans * 4, transcendentals=0
        ),
        name="norm",
    )(pair, gain, shift)


def weight(mine_ref, other_ref, n):
    mine, other = mine_ref[n], other_ref[n]
    first = lax.axis_index("col") == 0
    return jnp.concatenate([jnp.where(first, mine, other), jnp.where(first, other, mine)], axis=0)


def side_kernel(side, lag, mask_sref, normed_ref, maskk_ref, mine_ref, other_ref, b_ref, out_ref, stage):
    rows, length, chans = normed_ref.shape
    chips, share = out_ref.shape[:2]
    width = stage.shape[1]
    pitch = stage.shape[0] // chips
    core = lax.axis_index("col")
    if lag:
        pl.when(core == 1)(lambda: pl.delay(lag))
    base = (lax.axis_index("row") * lax.axis_size("col") + core) * rows
    bias = jnp.transpose(jnp.concatenate([b_ref[...], jnp.zeros((3, chans), F32)], axis=0))
    w_value = weight(mine_ref, other_ref, 2 * side)
    w_gate = weight(mine_ref, other_ref, 2 * side + 1)
    for k in range(length // width):
        normed = normed_ref[:, k * width : (k + 1) * width, :].reshape(rows * width, chans)
        value = dot(w_value, normed, NT) + bias[:, 2 * side : 2 * side + 1]
        gate = dot(w_gate, normed, NT) + bias[:, 2 * side + 1 : 2 * side + 2]
        value = jax.nn.sigmoid(gate) * value
        mask_k = maskk_ref[:, k * width : (k + 1) * width].astype(F32)
        for r in range(rows):
            part = value[:, r * width : (r + 1) * width] * (mask_k * mask_sref[base + r].astype(F32))
            for c in range(share):
                stage[pl.ds(c * rows + r, chips, stride=pitch), :] = part[c * chips : (c + 1) * chips]
        for z in range(chips):
            block = stage[z * pitch : z * pitch + share * rows, :].reshape(share, rows, width)
            out_ref[z, :, :, k * width : (k + 1) * width] = block.astype(BF16)


def make_side(side, lag, normed, mask, w_mine, w_other, b_in, chips):
    rows, length, chans = normed.shape
    share = chans // chips
    return pl.pallas_call(
        functools.partial(side_kernel, side, lag),
        in_specs=[pl.BlockSpec(memory_space=pltpu.SMEM)] + [in_vmem()] * 5,
        out_specs=in_vmem(),
        out_shape=jax.ShapeDtypeStruct((chips, share, rows, length), BF16),
        scratch_shapes=[pltpu.VMEM((chips * (share * rows + 8), 128), F32)],
        cost_estimate=pl.CostEstimate(
            flops=4 * rows * length * chans * chans, bytes_accessed=rows * length * chans * 4, transcendentals=0
        ),
        name=("left", "right")[side],
    )(mask, normed, mask.reshape(1, length), w_mine, w_other, b_in)


def gate_kernel(normed_ref, mine_ref, other_ref, b_ref, out_ref):
    normed = normed_ref[pl.program_id(0)]
    pre = dot(normed, weight(mine_ref, other_ref, 4), NT) + b_ref[4:5]
    out_ref[0] = jax.nn.sigmoid(pre)


def make_gate(normed, w_mine, w_other, b_in):
    rows, length, chans = normed.shape
    return pl.pallas_call(
        gate_kernel,
        grid=(rows,),
        in_specs=[in_vmem()] * 4,
        out_specs=pl.BlockSpec((1, length, chans), lambda r: (r, 0, 0)),
        out_shape=jax.ShapeDtypeStruct((rows, length, chans), F32),
        cost_estimate=pl.CostEstimate(
            flops=2 * rows * length * chans * chans, bytes_accessed=rows * length * chans * 6, transcendentals=0
        ),
        name="gate",
    )(normed, w_mine, w_other, b_in)


def triangle_kernel(left_ref, right_ref, other_ref, out_ref):
    chips, share, rows, length = left_ref.shape
    half = chips * rows
    core = lax.axis_index("col")
    for c in range(share):
        left = left_ref[:, c].reshape(half, length)
        mine = right_ref[:, c].reshape(half, length)
        other = other_ref[:, c].reshape(half, length)
        first = jnp.where(core == 0, mine, other)
        second = jnp.where(core == 0, other, mine)
        out_ref[:, c, :, 0:half] = dot(left, first, NT).astype(BF16).reshape(chips, rows, half)
        out_ref[:, c, :, half : 2 * half] = dot(left, second, NT).astype(BF16).reshape(chips, rows, half)


def make_triangle(left, right, other):
    return pl.pallas_call(
        triangle_kernel,
        in_specs=[in_vmem()] * 3,
        out_specs=in_vmem(),
        out_shape=jax.ShapeDtypeStruct(left.shape, BF16),
        name="triangle",
    )(*pinned(left), right, *pinned(other))


def finish_kernel(
    prod_ref,
    gate_ref,
    pair_ref,
    w_ref,
    b_ref,
    cols_ref,
    headt_ref,
    headb_ref,
    headbt_ref,
    update_ref,
    send_ref,
    own_ref,
    stage,
    sendst,
):
    chans, rows, _ = prod_ref.shape
    width = stage.shape[2]
    bins = headt_ref.shape[0]
    near = update_ref.shape[1]
    step, steps = pl.program_id(0), pl.num_programs(0)
    gain, shift = cols_ref[:, 0:1], cols_ref[:, 1:2]
    head_t = headt_ref[...]
    head_two = jnp.concatenate([head_t, head_t], axis=0)
    flat = (rows * width, chans)
    logits = []
    for t in range(2):
        at = pl.multiple_of((t * steps + step) * width, width)
        x = prod_ref[:, :, pl.ds(at, width)].astype(F32)
        centred = x - jnp.mean(x, axis=0, keepdims=True)
        spread = jnp.mean(centred * centred, axis=0, keepdims=True)
        stage[t] = (centred * lax.rsqrt(spread + 1.0)).reshape(chans * rows, width)
        normed = [stage[t, pl.ds(r, chans, stride=rows), :] * gain + shift for r in range(rows)]
        normed = jnp.concatenate(normed, axis=1).astype(BF16)
        mixed = dot(normed, w_ref[...], TN) + b_ref[...]
        update = (gate_ref[:, :, t].reshape(flat) * mixed).astype(BF16)
        update_ref[:, :, t] = update.reshape(rows, near, rows, chans)
        pair = pair_ref[:, :, t].reshape(flat)
        new_pair = (pair.astype(F32) + update.astype(F32)).astype(BF16)
        own = dot(head_t, new_pair, NT) + headbt_ref[...]
        for r in range(rows):
            own_ref[t * steps + step, pl.ds(r, bins, stride=rows), :] = own[:, r * width : (r + 1) * width]
        logits.append(dot(new_pair, head_two, NT) + headb_ref[...])
    lane = lax.broadcasted_iota(jnp.int32, logits[0].shape, 1)
    both = jnp.where(lane < bins, logits[0], logits[1])
    for r in range(rows):
        sendst[pl.ds(r, width, stride=rows), :] = both[r * width : (r + 1) * width]
    send_ref[pl.ds(step * near, near)] = sendst[...].reshape(near, rows, rows, 2 * bins).astype(BF16)


def make_finish(prod, gate, pair, w_out, b_out, cols, head_w, head_b):
    chips = prod.shape[0]
    rows, length, chans = pair.shape
    bins = head_w.shape[1]
    cores = 2
    width = 128
    steps = length // (cores * width)
    near = chips // steps
    prod = prod.reshape(chans, rows, length)
    view = (rows, chips, cores, rows, chans)
    wide = pl.BlockSpec((rows, near, cores, rows, chans), lambda z: (0, z, 0, 0, 0))
    head_row = jnp.concatenate([head_b, head_b]).reshape(1, 2 * bins)
    update, send, own = pl.pallas_call(
        finish_kernel,
        grid=(steps,),
        in_specs=[
            in_vmem(),
            wide,
            wide,
            whole(*w_out.shape),
            whole(1, chans),
            whole(*cols.shape),
            whole(bins, chans),
            whole(1, 2 * bins),
            whole(bins, 1),
        ],
        out_specs=[wide, in_vmem(), in_vmem()],
        out_shape=[
            jax.ShapeDtypeStruct(view, BF16),
            jax.ShapeDtypeStruct((chips, rows, rows, 2 * bins), BF16),
            jax.ShapeDtypeStruct((length // width, bins * rows, width), F32),
        ],
        scratch_shapes=[
            pltpu.VMEM((2, chans * rows, width), F32),
            pltpu.VMEM((near * rows * rows, 2 * bins), F32),
        ],
        name="finish",
    )(
        *pinned(prod),
        gate.reshape(view),
        pair.reshape(view),
        w_out,
        b_out.reshape(1, chans),
        cols,
        jnp.transpose(head_w),
        head_row,
        head_b.reshape(bins, 1),
    )
    return update.reshape(rows, length, chans), send, own


def loss_kernel(mask_sref, own_ref, mine_ref, other_ref, targets_ref, maskk_ref, out_ref, stage):
    chips, rows, _, lanes = mine_ref.shape
    bins = lanes // 2
    half = chips * rows
    length = 2 * half
    core = lax.axis_index("col")
    base = (lax.axis_index("row") * lax.axis_size("col") + core) * rows
    pick_row = lax.broadcasted_iota(jnp.int32, (bins, lanes), 0) + core * bins
    pick = jnp.where(pick_row == lax.broadcasted_iota(jnp.int32, (bins, lanes), 1), 1.0, 0.0).astype(BF16)
    for r in range(rows):
        at = pl.ds(r, bins, stride=rows)
        mine = dot(pick, mine_ref[:, r].reshape(half, lanes), NT)
        other = dot(pick, other_ref[:, r].reshape(half, lanes), NT)
        first = jnp.where(core == 0, mine, other)
        second = jnp.where(core == 0, other, mine)
        for q in range(half // 128):
            stage[q, at, :] = first[:, q * 128 : (q + 1) * 128]
            stage[half // 128 + q, at, :] = second[:, q * 128 : (q + 1) * 128]
    symmetric = jnp.concatenate([own_ref[q] + stage[q] for q in range(length // 128)], axis=1)
    symmetric = symmetric.reshape(bins, rows, length)
    top = jnp.max(symmetric, axis=0)
    total = jnp.sum(jnp.exp(symmetric - top[None]), axis=0)
    bin_index = lax.broadcasted_iota(jnp.int32, (bins, rows, length), 0)
    picked = jnp.sum(jnp.where(targets_ref[...][None] == bin_index, symmetric, 0.0), axis=0)
    loss = top + jnp.log(total) - picked
    high = loss.astype(BF16)
    rest = loss - high.astype(F32)
    middle = rest.astype(BF16)
    low = (rest - middle.astype(F32)).astype(BF16)
    spot = lax.broadcasted_iota(jnp.int32, (length, length), 0)
    place = lax.broadcasted_iota(jnp.int32, (length, length), 1)
    come = (place // rows % 2) * half + (place // (2 * rows)) * rows + place % rows
    order = jnp.where(spot == come, 1.0, 0.0).astype(BF16)
    natural = dot(high, order, (((1,), (0,)), ((), ())))
    natural += dot(middle, order, (((1,), (0,)), ((), ())))
    natural += dot(low, order, (((1,), (0,)), ((), ())))
    row = lax.broadcasted_iota(jnp.int32, (rows, length), 0)
    mask_i = jnp.zeros((rows, length), F32)
    for r in range(rows):
        mask_i = jnp.where(row == r, mask_sref[base + r].astype(F32), mask_i)
    out_ref[...] = mask_i * maskk_ref[...].astype(F32) * natural


def make_loss(mask, own, mine, other, targets):
    rows, length = targets.shape
    return pl.pallas_call(
        loss_kernel,
        in_specs=[pl.BlockSpec(memory_space=pltpu.SMEM)] + [in_vmem()] * 5,
        out_specs=in_vmem(),
        out_shape=jax.ShapeDtypeStruct((rows, length), F32),
        scratch_shapes=[pltpu.VMEM(own.shape, F32)],
        name="loss",
    )(mask, own, *pinned(mine, other), targets, mask.reshape(1, length))


LAG_NS = 35000


def local(
    pair, residue_mask, targets, ln_gain, ln_shift, w_in, b_in, w_out, b_out, head_weight, head_bias
):
    rows, length, chans = pair.shape
    chips = lax.axis_size("row")
    share = chans // chips
    swap = functools.partial(lax.ppermute, axis_name="col", perm=[(0, 1), (1, 0)])
    exchange = lambda v: lax.all_to_all(v, "row", split_axis=0, concat_axis=0, tiled=True)
    by_owner = lambda v: jnp.swapaxes(v.reshape(share, chips, -1), 0, 1).reshape(chans, -1)
    w_mine = jnp.transpose(w_in, (0, 2, 1))
    w_other = swap(w_mine)
    out_other = swap(w_out)
    normed = make_norm(pair, ln_gain, ln_shift)
    right = make_side(1, LAG_NS, normed, residue_mask, w_mine, *pinned(w_other), b_in, chips)
    right, out_other = lax.optimization_barrier((right, out_other))
    right = exchange(right)
    left = make_side(0, 0, normed, residue_mask, w_mine, w_other, b_in, chips)
    gate = make_gate(normed, w_mine, w_other, b_in)
    first = lax.axis_index("col") == 0
    w_full = jnp.concatenate([jnp.where(first, w_out, out_other), jnp.where(first, out_other, w_out)], axis=0)
    w_full = by_owner(w_full)
    cols = by_owner(jnp.stack([ln_gain[1], ln_shift[1]], axis=1))
    targets = jnp.swapaxes(targets.reshape(rows, chips, 2, rows), 1, 2).reshape(rows, length)
    left, targets, w_full, cols = lax.optimization_barrier((left, targets, w_full, cols))
    right_other = swap(right)
    left = exchange(left)
    product = exchange(make_triangle(left, right, right_other))
    update, send, own = make_finish(product, gate, pair, w_full, b_out, cols, head_weight, head_bias)
    mine = exchange(send)
    loss = make_loss(residue_mask, own, mine, swap(mine), targets)
    return (update, loss)


def solution(mesh):
    placed = (
        P(("ga", "row", "col"), None, None),
        P("ga"),
        P(("ga", "row", "col"), None),
        P(),
        P(),
        P(None, None, "col"),
        P(),
        P("col", None),
        P(),
        P(),
        P(),
    )
    return jax.shard_map(
        local,
        mesh=mesh,
        in_specs=placed,
        out_specs=(P(("ga", "row", "col"), None, None), P(("ga", "row", "col"), None)),
        check_vma=False,
    )
```

```python
import functools

import jax
import jax.numpy as jnp
from jax import lax
from jax.experimental import pallas as pl
from jax.experimental.pallas import tpu as pltpu
from jax.sharding import PartitionSpec as P

F32 = jnp.float32
BF16 = jnp.bfloat16
NT = (((1,), (1,)), ((), ()))
TN = (((0,), (0,)), ((), ()))


def dot(a, b, dims):
    return lax.dot_general(a, b, dims, preferred_element_type=F32)


def whole(*shape):
    return pl.BlockSpec(shape, lambda *_: (0,) * len(shape))


def in_vmem():
    return pl.BlockSpec(memory_space=pltpu.VMEM)


def pinned(*arrays):
    return [pltpu.with_memory_space_constraint(a, pltpu.VMEM) for a in arrays]


def norm_kernel(pair_ref, gain_ref, shift_ref, out_ref):
    chans = pair_ref.shape[-1]
    pair = pair_ref[...].reshape(-1, chans)
    centred = pair.astype(F32) - dot(pair, jnp.full((chans, chans), 1.0 / chans, BF16), NT)
    spread = jnp.mean(centred * centred, axis=-1, keepdims=True)
    normed = centred * lax.rsqrt(spread + 0.1) * gain_ref[0:1] + shift_ref[0:1]
    rows = pair_ref.shape[0]
    out_ref[pl.ds(pl.program_id(0) * rows, rows)] = normed.astype(BF16).reshape(pair_ref.shape)


def make_norm(pair, gain, shift):
    rows, length, chans = pair.shape
    return pl.pallas_call(
        norm_kernel,
        grid=(rows // 2,),
        in_specs=[
            pl.BlockSpec((2, length, chans), lambda r: (r, 0, 0)),
            whole(*gain.shape),
            whole(*shift.shape),
        ],
        out_specs=in_vmem(),
        out_shape=jax.ShapeDtypeStruct(pair.shape, BF16),
        cost_estimate=pl.CostEstimate(
            flops=rows * length * chans * 100, bytes_accessed=rows * length * chans * 4, transcendentals=0
        ),
        name="norm",
    )(pair, gain, shift)


def weight(mine_ref, other_ref, n):
    mine, other = mine_ref[n], other_ref[n]
    first = lax.axis_index("col") == 0
    return jnp.concatenate([jnp.where(first, mine, other), jnp.where(first, other, mine)], axis=0)


def side_kernel(side, lag, mask_sref, normed_ref, maskk_ref, mine_ref, other_ref, b_ref, out_ref, stage):
    rows, length, chans = normed_ref.shape
    chips, share = out_ref.shape[:2]
    width = stage.shape[1]
    pitch = stage.shape[0] // chips
    core = lax.axis_index("col")
    if lag:
        pl.when(core == 1)(lambda: pl.delay(lag))
    base = (lax.axis_index("row") * lax.axis_size("col") + core) * rows
    bias = jnp.transpose(jnp.concatenate([b_ref[...], jnp.zeros((3, chans), F32)], axis=0))
    w_value = weight(mine_ref, other_ref, 2 * side)
    w_gate = weight(mine_ref, other_ref, 2 * side + 1)
    for k in range(length // width):
        normed = normed_ref[:, k * width : (k + 1) * width, :].reshape(rows * width, chans)
        value = dot(w_value, normed, NT) + bias[:, 2 * side : 2 * side + 1]
        gate = dot(w_gate, normed, NT) + bias[:, 2 * side + 1 : 2 * side + 2]
        value = jax.nn.sigmoid(gate) * value
        mask_k = maskk_ref[:, k * width : (k + 1) * width].astype(F32)
        for r in range(rows):
            part = value[:, r * width : (r + 1) * width] * (mask_k * mask_sref[base + r].astype(F32))
            for c in range(share):
                stage[pl.ds(c * rows + r, chips, stride=pitch), :] = part[c * chips : (c + 1) * chips]
        for z in range(chips):
            block = stage[z * pitch : z * pitch + share * rows, :].reshape(share, rows, width)
            out_ref[z, :, :, k * width : (k + 1) * width] = block.astype(BF16)


def make_side(side, lag, normed, mask, w_mine, w_other, b_in, chips):
    rows, length, chans = normed.shape
    share = chans // chips
    return pl.pallas_call(
        functools.partial(side_kernel, side, lag),
        in_specs=[pl.BlockSpec(memory_space=pltpu.SMEM)] + [in_vmem()] * 5,
        out_specs=in_vmem(),
        out_shape=jax.ShapeDtypeStruct((chips, share, rows, length), BF16),
        scratch_shapes=[pltpu.VMEM((chips * (share * rows + 8), 128), F32)],
        cost_estimate=pl.CostEstimate(
            flops=4 * rows * length * chans * chans, bytes_accessed=rows * length * chans * 4, transcendentals=0
        ),
        name=("left", "right")[side],
    )(mask, normed, mask.reshape(1, length), w_mine, w_other, b_in)


def gate_kernel(normed_ref, mine_ref, other_ref, b_ref, out_ref):
    normed = normed_ref[pl.program_id(0)]
    pre = dot(normed, weight(mine_ref, other_ref, 4), NT) + b_ref[4:5]
    out_ref[0] = jax.nn.sigmoid(pre)


def make_gate(normed, w_mine, w_other, b_in):
    rows, length, chans = normed.shape
    return pl.pallas_call(
        gate_kernel,
        grid=(rows,),
        in_specs=[in_vmem()] * 4,
        out_specs=pl.BlockSpec((1, length, chans), lambda r: (r, 0, 0)),
        out_shape=jax.ShapeDtypeStruct((rows, length, chans), F32),
        cost_estimate=pl.CostEstimate(
            flops=2 * rows * length * chans * chans, bytes_accessed=rows * length * chans * 6, transcendentals=0
        ),
        name="gate",
    )(normed, w_mine, w_other, b_in)


def triangle_kernel(left_ref, right_ref, other_ref, out_ref):
    chips, share, rows, length = left_ref.shape
    half = chips * rows
    core = lax.axis_index("col")
    for c in range(share):
        left = left_ref[:, c].reshape(half, length)
        mine = right_ref[:, c].reshape(half, length)
        other = other_ref[:, c].reshape(half, length)
        first = jnp.where(core == 0, mine, other)
        second = jnp.where(core == 0, other, mine)
        out_ref[:, c, :, 0:half] = dot(left, first, NT).astype(BF16).reshape(chips, rows, half)
        out_ref[:, c, :, half : 2 * half] = dot(left, second, NT).astype(BF16).reshape(chips, rows, half)


def make_triangle(left, right, other):
    return pl.pallas_call(
        triangle_kernel,
        in_specs=[in_vmem()] * 3,
        out_specs=in_vmem(),
        out_shape=jax.ShapeDtypeStruct(left.shape, BF16),
        name="triangle",
    )(*pinned(left), right, *pinned(other))


def finish_kernel(
    prod_ref,
    gate_ref,
    pair_ref,
    w_ref,
    b_ref,
    cols_ref,
    headt_ref,
    headb_ref,
    headbt_ref,
    update_ref,
    send_ref,
    own_ref,
    stage,
    sendst,
):
    chans, rows, _ = prod_ref.shape
    width = stage.shape[2]
    bins = headt_ref.shape[0]
    near = update_ref.shape[1]
    step, steps = pl.program_id(0), pl.num_programs(0)
    gain, shift = cols_ref[:, 0:1], cols_ref[:, 1:2]
    head_t = headt_ref[...]
    head_two = jnp.concatenate([head_t, head_t], axis=0)
    flat = (rows * width, chans)
    logits = []
    for t in range(2):
        at = pl.multiple_of((t * steps + step) * width, width)
        x = prod_ref[:, :, pl.ds(at, width)].astype(F32)
        centred = x - jnp.mean(x, axis=0, keepdims=True)
        spread = jnp.mean(centred * centred, axis=0, keepdims=True)
        stage[t] = (centred * lax.rsqrt(spread + 1.0)).reshape(chans * rows, width)
        normed = [stage[t, pl.ds(r, chans, stride=rows), :] * gain + shift for r in range(rows)]
        normed = jnp.concatenate(normed, axis=1).astype(BF16)
        mixed = dot(normed, w_ref[...], TN) + b_ref[...]
        update = (gate_ref[:, :, t].reshape(flat) * mixed).astype(BF16)
        update_ref[:, :, t] = update.reshape(rows, near, rows, chans)
        pair = pair_ref[:, :, t].reshape(flat)
        new_pair = (pair.astype(F32) + update.astype(F32)).astype(BF16)
        own = dot(head_t, new_pair, NT) + headbt_ref[...]
        for r in range(rows):
            own_ref[t * steps + step, pl.ds(r, bins, stride=rows), :] = own[:, r * width : (r + 1) * width]
        logits.append(dot(new_pair, head_two, NT) + headb_ref[...])
    lane = lax.broadcasted_iota(jnp.int32, logits[0].shape, 1)
    both = jnp.where(lane < bins, logits[0], logits[1])
    for r in range(rows):
        sendst[pl.ds(r, width, stride=rows), :] = both[r * width : (r + 1) * width]
    send_ref[pl.ds(step * near, near)] = sendst[...].reshape(near, rows, rows, 2 * bins).astype(BF16)


def make_finish(prod, gate, pair, w_out, b_out, cols, head_w, head_b):
    chips = prod.shape[0]
    rows, length, chans = pair.shape
    bins = head_w.shape[1]
    cores = 2
    width = 128
    steps = length // (cores * width)
    near = chips // steps
    prod = prod.reshape(chans, rows, length)
    view = (rows, chips, cores, rows, chans)
    wide = pl.BlockSpec((rows, near, cores, rows, chans), lambda z: (0, z, 0, 0, 0))
    head_row = jnp.concatenate([head_b, head_b]).reshape(1, 2 * bins)
    update, send, own = pl.pallas_call(
        finish_kernel,
        grid=(steps,),
        in_specs=[
            in_vmem(),
            wide,
            wide,
            whole(*w_out.shape),
            whole(1, chans),
            whole(*cols.shape),
            whole(bins, chans),
            whole(1, 2 * bins),
            whole(bins, 1),
        ],
        out_specs=[wide, in_vmem(), in_vmem()],
        out_shape=[
            jax.ShapeDtypeStruct(view, BF16),
            jax.ShapeDtypeStruct((chips, rows, rows, 2 * bins), BF16),
            jax.ShapeDtypeStruct((length // width, bins * rows, width), F32),
        ],
        scratch_shapes=[
            pltpu.VMEM((2, chans * rows, width), F32),
            pltpu.VMEM((near * rows * rows, 2 * bins), F32),
        ],
        name="finish",
    )(
        *pinned(prod),
        gate.reshape(view),
        pair.reshape(view),
        w_out,
        b_out.reshape(1, chans),
        cols,
        jnp.transpose(head_w),
        head_row,
        head_b.reshape(bins, 1),
    )
    return update.reshape(rows, length, chans), send, own


def loss_kernel(mask_sref, own_ref, mine_ref, other_ref, targets_ref, maskk_ref, out_ref, stage):
    chips, rows, _, lanes = mine_ref.shape
    bins = lanes // 2
    half = chips * rows
    length = 2 * half
    core = lax.axis_index("col")
    base = (lax.axis_index("row") * lax.axis_size("col") + core) * rows
    pick_row = lax.broadcasted_iota(jnp.int32, (bins, lanes), 0) + core * bins
    pick = jnp.where(pick_row == lax.broadcasted_iota(jnp.int32, (bins, lanes), 1), 1.0, 0.0).astype(BF16)
    for r in range(rows):
        at = pl.ds(r, bins, stride=rows)
        mine = dot(pick, mine_ref[:, r].reshape(half, lanes), NT)
        other = dot(pick, other_ref[:, r].reshape(half, lanes), NT)
        first = jnp.where(core == 0, mine, other)
        second = jnp.where(core == 0, other, mine)
        for q in range(half // 128):
            stage[q, at, :] = first[:, q * 128 : (q + 1) * 128]
            stage[half // 128 + q, at, :] = second[:, q * 128 : (q + 1) * 128]
    symmetric = jnp.concatenate([own_ref[q] + stage[q] for q in range(length // 128)], axis=1)
    symmetric = symmetric.reshape(bins, rows, length)
    top = jnp.max(symmetric, axis=0)
    total = jnp.sum(jnp.exp(symmetric - top[None]), axis=0)
    bin_index = lax.broadcasted_iota(jnp.int32, (bins, rows, length), 0)
    picked = jnp.sum(jnp.where(targets_ref[...][None] == bin_index, symmetric, 0.0), axis=0)
    loss = top + jnp.log(total) - picked
    high = loss.astype(BF16)
    rest = loss - high.astype(F32)
    middle = rest.astype(BF16)
    low = (rest - middle.astype(F32)).astype(BF16)
    spot = lax.broadcasted_iota(jnp.int32, (length, length), 0)
    place = lax.broadcasted_iota(jnp.int32, (length, length), 1)
    come = (place // rows % 2) * half + (place // (2 * rows)) * rows + place % rows
    order = jnp.where(spot == come, 1.0, 0.0).astype(BF16)
    natural = dot(high, order, (((1,), (0,)), ((), ())))
    natural += dot(middle, order, (((1,), (0,)), ((), ())))
    natural += dot(low, order, (((1,), (0,)), ((), ())))
    row = lax.broadcasted_iota(jnp.int32, (rows, length), 0)
    mask_i = jnp.zeros((rows, length), F32)
    for r in range(rows):
        mask_i = jnp.where(row == r, mask_sref[base + r].astype(F32), mask_i)
    out_ref[...] = mask_i * maskk_ref[...].astype(F32) * natural


def make_loss(mask, own, mine, other, targets):
    rows, length = targets.shape
    return pl.pallas_call(
        loss_kernel,
        in_specs=[pl.BlockSpec(memory_space=pltpu.SMEM)] + [in_vmem()] * 5,
        out_specs=in_vmem(),
        out_shape=jax.ShapeDtypeStruct((rows, length), F32),
        scratch_shapes=[pltpu.VMEM(own.shape, F32)],
        name="loss",
    )(mask, own, *pinned(mine, other), targets, mask.reshape(1, length))


LAG_NS = 39000


def local(
    pair, residue_mask, targets, ln_gain, ln_shift, w_in, b_in, w_out, b_out, head_weight, head_bias
):
    rows, length, chans = pair.shape
    chips = lax.axis_size("row")
    share = chans // chips
    swap = functools.partial(lax.ppermute, axis_name="col", perm=[(0, 1), (1, 0)])
    exchange = lambda v: lax.all_to_all(v, "row", split_axis=0, concat_axis=0, tiled=True)
    by_owner = lambda v: jnp.swapaxes(v.reshape(share, chips, -1), 0, 1).reshape(chans, -1)
    w_mine = jnp.transpose(w_in, (0, 2, 1))
    w_other = swap(w_mine)
    out_other = swap(w_out)
    normed = make_norm(pair, ln_gain, ln_shift)
    right = make_side(1, LAG_NS, normed, residue_mask, w_mine, *pinned(w_other), b_in, chips)
    right, out_other = lax.optimization_barrier((right, out_other))
    right = exchange(right)
    left = make_side(0, 0, normed, residue_mask, w_mine, w_other, b_in, chips)
    gate = make_gate(normed, w_mine, w_other, b_in)
    first = lax.axis_index("col") == 0
    w_full = jnp.concatenate([jnp.where(first, w_out, out_other), jnp.where(first, out_other, w_out)], axis=0)
    w_full = by_owner(w_full)
    cols = by_owner(jnp.stack([ln_gain[1], ln_shift[1]], axis=1))
    targets = jnp.swapaxes(targets.reshape(rows, chips, 2, rows), 1, 2).reshape(rows, length)
    left, targets, w_full, cols = lax.optimization_barrier((left, targets, w_full, cols))
    right_other = swap(right)
    left = exchange(left)
    product = exchange(make_triangle(left, right, right_other))
    update, send, own = make_finish(product, gate, pair, w_full, b_out, cols, head_weight, head_bias)
    mine = exchange(send)
    loss = make_loss(residue_mask, own, mine, swap(mine), targets)
    return (update, loss)


def solution(mesh):
    placed = (
        P(("ga", "row", "col"), None, None),
        P("ga"),
        P(("ga", "row", "col"), None),
        P(),
        P(),
        P(None, None, "col"),
        P(),
        P("col", None),
        P(),
        P(),
        P(),
    )
    return jax.shard_map(
        local,
        mesh=mesh,
        in_specs=placed,
        out_specs=(P(("ga", "row", "col"), None, None), P(("ga", "row", "col"), None)),
        check_vma=False,
    )
```

```python
import functools

import jax
import jax.numpy as jnp
from jax import lax
from jax.experimental import pallas as pl
from jax.experimental.pallas import tpu as pltpu
from jax.sharding import PartitionSpec as P

F32 = jnp.float32
BF16 = jnp.bfloat16
NT = (((1,), (1,)), ((), ()))
TN = (((0,), (0,)), ((), ()))


def dot(a, b, dims):
    return lax.dot_general(a, b, dims, preferred_element_type=F32)


def whole(*shape):
    return pl.BlockSpec(shape, lambda *_: (0,) * len(shape))


def in_vmem():
    return pl.BlockSpec(memory_space=pltpu.VMEM)


def pinned(*arrays):
    return [pltpu.with_memory_space_constraint(a, pltpu.VMEM) for a in arrays]


def norm_kernel(pair_ref, gain_ref, shift_ref, out_ref):
    chans = pair_ref.shape[-1]
    pair = pair_ref[...].reshape(-1, chans)
    centred = pair.astype(F32) - dot(pair, jnp.full((chans, chans), 1.0 / chans, BF16), NT)
    spread = jnp.mean(centred * centred, axis=-1, keepdims=True)
    normed = centred * lax.rsqrt(spread + 0.1) * gain_ref[0:1] + shift_ref[0:1]
    rows = pair_ref.shape[0]
    out_ref[pl.ds(pl.program_id(0) * rows, rows)] = normed.astype(BF16).reshape(pair_ref.shape)


def make_norm(pair, gain, shift):
    rows, length, chans = pair.shape
    return pl.pallas_call(
        norm_kernel,
        grid=(rows // 2,),
        in_specs=[
            pl.BlockSpec((2, length, chans), lambda r: (r, 0, 0)),
            whole(*gain.shape),
            whole(*shift.shape),
        ],
        out_specs=in_vmem(),
        out_shape=jax.ShapeDtypeStruct(pair.shape, BF16),
        cost_estimate=pl.CostEstimate(
            flops=rows * length * chans * 100, bytes_accessed=rows * length * chans * 4, transcendentals=0
        ),
        name="norm",
    )(pair, gain, shift)


def weight(mine_ref, other_ref, n):
    mine, other = mine_ref[n], other_ref[n]
    first = lax.axis_index("col") == 0
    return jnp.concatenate([jnp.where(first, mine, other), jnp.where(first, other, mine)], axis=0)


def side_kernel(side, lag, mask_sref, normed_ref, maskk_ref, mine_ref, other_ref, b_ref, out_ref, stage):
    rows, length, chans = normed_ref.shape
    chips, share = out_ref.shape[:2]
    width = stage.shape[1]
    pitch = stage.shape[0] // chips
    core = lax.axis_index("col")
    if lag:
        pl.when(core == 1)(lambda: pl.delay(lag))
    base = (lax.axis_index("row") * lax.axis_size("col") + core) * rows
    bias = jnp.transpose(jnp.concatenate([b_ref[...], jnp.zeros((3, chans), F32)], axis=0))
    w_value = weight(mine_ref, other_ref, 2 * side)
    w_gate = weight(mine_ref, other_ref, 2 * side + 1)
    for k in range(length // width):
        normed = normed_ref[:, k * width : (k + 1) * width, :].reshape(rows * width, chans)
        value = dot(w_value, normed, NT) + bias[:, 2 * side : 2 * side + 1]
        gate = dot(w_gate, normed, NT) + bias[:, 2 * side + 1 : 2 * side + 2]
        value = jax.nn.sigmoid(gate) * value
        mask_k = maskk_ref[:, k * width : (k + 1) * width].astype(F32)
        for r in range(rows):
            part = value[:, r * width : (r + 1) * width] * (mask_k * mask_sref[base + r].astype(F32))
            for c in range(share):
                stage[pl.ds(c * rows + r, chips, stride=pitch), :] = part[c * chips : (c + 1) * chips]
        for z in range(chips):
            block = stage[z * pitch : z * pitch + share * rows, :].reshape(share, rows, width)
            out_ref[z, :, :, k * width : (k + 1) * width] = block.astype(BF16)


def make_side(side, lag, normed, mask, w_mine, w_other, b_in, chips):
    rows, length, chans = normed.shape
    share = chans // chips
    return pl.pallas_call(
        functools.partial(side_kernel, side, lag),
        in_specs=[pl.BlockSpec(memory_space=pltpu.SMEM)] + [in_vmem()] * 5,
        out_specs=in_vmem(),
        out_shape=jax.ShapeDtypeStruct((chips, share, rows, length), BF16),
        scratch_shapes=[pltpu.VMEM((chips * (share * rows + 8), 128), F32)],
        cost_estimate=pl.CostEstimate(
            flops=4 * rows * length * chans * chans, bytes_accessed=rows * length * chans * 4, transcendentals=0
        ),
        name=("left", "right")[side],
    )(mask, normed, mask.reshape(1, length), w_mine, w_other, b_in)


def gate_kernel(normed_ref, mine_ref, other_ref, b_ref, out_ref):
    normed = normed_ref[pl.program_id(0)]
    pre = dot(normed, weight(mine_ref, other_ref, 4), NT) + b_ref[4:5]
    out_ref[0] = jax.nn.sigmoid(pre)


def make_gate(normed, w_mine, w_other, b_in):
    rows, length, chans = normed.shape
    return pl.pallas_call(
        gate_kernel,
        grid=(rows,),
        in_specs=[in_vmem()] * 4,
        out_specs=pl.BlockSpec((1, length, chans), lambda r: (r, 0, 0)),
        out_shape=jax.ShapeDtypeStruct((rows, length, chans), F32),
        cost_estimate=pl.CostEstimate(
            flops=2 * rows * length * chans * chans, bytes_accessed=rows * length * chans * 6, transcendentals=0
        ),
        name="gate",
    )(normed, w_mine, w_other, b_in)


def triangle_kernel(left_ref, right_ref, other_ref, out_ref):
    chips, share, rows, length = left_ref.shape
    half = chips * rows
    core = lax.axis_index("col")
    for c in range(share):
        left = left_ref[:, c].reshape(half, length)
        mine = right_ref[:, c].reshape(half, length)
        other = other_ref[:, c].reshape(half, length)
        first = jnp.where(core == 0, mine, other)
        second = jnp.where(core == 0, other, mine)
        out_ref[:, c, :, 0:half] = dot(left, first, NT).astype(BF16).reshape(chips, rows, half)
        out_ref[:, c, :, half : 2 * half] = dot(left, second, NT).astype(BF16).reshape(chips, rows, half)


def make_triangle(left, right, other):
    return pl.pallas_call(
        triangle_kernel,
        in_specs=[in_vmem()] * 3,
        out_specs=in_vmem(),
        out_shape=jax.ShapeDtypeStruct(left.shape, BF16),
        name="triangle",
    )(*pinned(left), right, *pinned(other))


def finish_kernel(
    prod_ref,
    gate_ref,
    pair_ref,
    w_ref,
    b_ref,
    cols_ref,
    headt_ref,
    headb_ref,
    headbt_ref,
    update_ref,
    send_ref,
    own_ref,
    stage,
    sendst,
):
    chans, rows, _ = prod_ref.shape
    width = stage.shape[2]
    bins = headt_ref.shape[0]
    near = update_ref.shape[1]
    step, steps = pl.program_id(0), pl.num_programs(0)
    gain, shift = cols_ref[:, 0:1], cols_ref[:, 1:2]
    head_t = headt_ref[...]
    head_two = jnp.concatenate([head_t, head_t], axis=0)
    flat = (rows * width, chans)
    logits = []
    for t in range(2):
        at = pl.multiple_of((t * steps + step) * width, width)
        x = prod_ref[:, :, pl.ds(at, width)].astype(F32)
        centred = x - jnp.mean(x, axis=0, keepdims=True)
        spread = jnp.mean(centred * centred, axis=0, keepdims=True)
        stage[t] = (centred * lax.rsqrt(spread + 1.0)).reshape(chans * rows, width)
        normed = [stage[t, pl.ds(r, chans, stride=rows), :] * gain + shift for r in range(rows)]
        normed = jnp.concatenate(normed, axis=1).astype(BF16)
        mixed = dot(normed, w_ref[...], TN) + b_ref[...]
        update = (gate_ref[:, :, t].reshape(flat) * mixed).astype(BF16)
        update_ref[:, :, t] = update.reshape(rows, near, rows, chans)
        pair = pair_ref[:, :, t].reshape(flat)
        new_pair = (pair.astype(F32) + update.astype(F32)).astype(BF16)
        own = dot(head_t, new_pair, NT) + headbt_ref[...]
        for r in range(rows):
            own_ref[t * steps + step, pl.ds(r, bins, stride=rows), :] = own[:, r * width : (r + 1) * width]
        logits.append(dot(new_pair, head_two, NT) + headb_ref[...])
    lane = lax.broadcasted_iota(jnp.int32, logits[0].shape, 1)
    both = jnp.where(lane < bins, logits[0], logits[1])
    for r in range(rows):
        sendst[pl.ds(r, width, stride=rows), :] = both[r * width : (r + 1) * width]
    send_ref[pl.ds(step * near, near)] = sendst[...].reshape(near, rows, rows, 2 * bins).astype(BF16)


def make_finish(prod, gate, pair, w_out, b_out, cols, head_w, head_b):
    chips = prod.shape[0]
    rows, length, chans = pair.shape
    bins = head_w.shape[1]
    cores = 2
    width = 128
    steps = length // (cores * width)
    near = chips // steps
    prod = prod.reshape(chans, rows, length)
    view = (rows, chips, cores, rows, chans)
    wide = pl.BlockSpec((rows, near, cores, rows, chans), lambda z: (0, z, 0, 0, 0))
    head_row = jnp.concatenate([head_b, head_b]).reshape(1, 2 * bins)
    update, send, own = pl.pallas_call(
        finish_kernel,
        grid=(steps,),
        in_specs=[
            in_vmem(),
            wide,
            wide,
            whole(*w_out.shape),
            whole(1, chans),
            whole(*cols.shape),
            whole(bins, chans),
            whole(1, 2 * bins),
            whole(bins, 1),
        ],
        out_specs=[wide, in_vmem(), in_vmem()],
        out_shape=[
            jax.ShapeDtypeStruct(view, BF16),
            jax.ShapeDtypeStruct((chips, rows, rows, 2 * bins), BF16),
            jax.ShapeDtypeStruct((length // width, bins * rows, width), F32),
        ],
        scratch_shapes=[
            pltpu.VMEM((2, chans * rows, width), F32),
            pltpu.VMEM((near * rows * rows, 2 * bins), F32),
        ],
        name="finish",
    )(
        *pinned(prod),
        gate.reshape(view),
        pair.reshape(view),
        w_out,
        b_out.reshape(1, chans),
        cols,
        jnp.transpose(head_w),
        head_row,
        head_b.reshape(bins, 1),
    )
    return update.reshape(rows, length, chans), send, own


def loss_kernel(mask_sref, own_ref, mine_ref, other_ref, targets_ref, maskk_ref, out_ref, stage):
    chips, rows, _, lanes = mine_ref.shape
    bins = lanes // 2
    half = chips * rows
    length = 2 * half
    core = lax.axis_index("col")
    base = (lax.axis_index("row") * lax.axis_size("col") + core) * rows
    pick_row = lax.broadcasted_iota(jnp.int32, (bins, lanes), 0) + core * bins
    pick = jnp.where(pick_row == lax.broadcasted_iota(jnp.int32, (bins, lanes), 1), 1.0, 0.0).astype(BF16)
    for r in range(rows):
        at = pl.ds(r, bins, stride=rows)
        mine = dot(pick, mine_ref[:, r].reshape(half, lanes), NT)
        other = dot(pick, other_ref[:, r].reshape(half, lanes), NT)
        first = jnp.where(core == 0, mine, other)
        second = jnp.where(core == 0, other, mine)
        for q in range(half // 128):
            stage[q, at, :] = first[:, q * 128 : (q + 1) * 128]
            stage[half // 128 + q, at, :] = second[:, q * 128 : (q + 1) * 128]
    symmetric = jnp.concatenate([own_ref[q] + stage[q] for q in range(length // 128)], axis=1)
    symmetric = symmetric.reshape(bins, rows, length)
    top = jnp.max(symmetric, axis=0)
    total = jnp.sum(jnp.exp(symmetric - top[None]), axis=0)
    bin_index = lax.broadcasted_iota(jnp.int32, (bins, rows, length), 0)
    picked = jnp.sum(jnp.where(targets_ref[...][None] == bin_index, symmetric, 0.0), axis=0)
    loss = top + jnp.log(total) - picked
    high = loss.astype(BF16)
    rest = loss - high.astype(F32)
    middle = rest.astype(BF16)
    low = (rest - middle.astype(F32)).astype(BF16)
    spot = lax.broadcasted_iota(jnp.int32, (length, length), 0)
    place = lax.broadcasted_iota(jnp.int32, (length, length), 1)
    come = (place // rows % 2) * half + (place // (2 * rows)) * rows + place % rows
    order = jnp.where(spot == come, 1.0, 0.0).astype(BF16)
    natural = dot(high, order, (((1,), (0,)), ((), ())))
    natural += dot(middle, order, (((1,), (0,)), ((), ())))
    natural += dot(low, order, (((1,), (0,)), ((), ())))
    row = lax.broadcasted_iota(jnp.int32, (rows, length), 0)
    mask_i = jnp.zeros((rows, length), F32)
    for r in range(rows):
        mask_i = jnp.where(row == r, mask_sref[base + r].astype(F32), mask_i)
    out_ref[...] = mask_i * maskk_ref[...].astype(F32) * natural


def make_loss(mask, own, mine, other, targets):
    rows, length = targets.shape
    return pl.pallas_call(
        loss_kernel,
        in_specs=[pl.BlockSpec(memory_space=pltpu.SMEM)] + [in_vmem()] * 5,
        out_specs=in_vmem(),
        out_shape=jax.ShapeDtypeStruct((rows, length), F32),
        scratch_shapes=[pltpu.VMEM(own.shape, F32)],
        name="loss",
    )(mask, own, *pinned(mine, other), targets, mask.reshape(1, length))


LAG_NS = 38000


def local(
    pair, residue_mask, targets, ln_gain, ln_shift, w_in, b_in, w_out, b_out, head_weight, head_bias
):
    rows, length, chans = pair.shape
    chips = lax.axis_size("row")
    share = chans // chips
    swap = functools.partial(lax.ppermute, axis_name="col", perm=[(0, 1), (1, 0)])
    exchange = lambda v: lax.all_to_all(v, "row", split_axis=0, concat_axis=0, tiled=True)
    by_owner = lambda v: jnp.swapaxes(v.reshape(share, chips, -1), 0, 1).reshape(chans, -1)
    w_mine = jnp.transpose(w_in, (0, 2, 1))
    w_other = swap(w_mine)
    out_other = swap(w_out)
    normed = make_norm(pair, ln_gain, ln_shift)
    right = make_side(1, LAG_NS, normed, residue_mask, w_mine, *pinned(w_other), b_in, chips)
    right, out_other = lax.optimization_barrier((right, out_other))
    right = exchange(right)
    left = make_side(0, 0, normed, residue_mask, w_mine, w_other, b_in, chips)
    gate = make_gate(normed, w_mine, w_other, b_in)
    first = lax.axis_index("col") == 0
    w_full = jnp.concatenate([jnp.where(first, w_out, out_other), jnp.where(first, out_other, w_out)], axis=0)
    w_full = by_owner(w_full)
    cols = by_owner(jnp.stack([ln_gain[1], ln_shift[1]], axis=1))
    targets = jnp.swapaxes(targets.reshape(rows, chips, 2, rows), 1, 2).reshape(rows, length)
    left, targets, w_full, cols = lax.optimization_barrier((left, targets, w_full, cols))
    right_other = swap(right)
    left = exchange(left)
    product = exchange(make_triangle(left, right, right_other))
    update, send, own = make_finish(product, gate, pair, w_full, b_out, cols, head_weight, head_bias)
    mine = exchange(send)
    loss = make_loss(residue_mask, own, mine, swap(mine), targets)
    return (update, loss)


def solution(mesh):
    placed = (
        P(("ga", "row", "col"), None, None),
        P("ga"),
        P(("ga", "row", "col"), None),
        P(),
        P(),
        P(None, None, "col"),
        P(),
        P("col", None),
        P(),
        P(),
        P(),
    )
    return jax.shard_map(
        local,
        mesh=mesh,
        in_specs=placed,
        out_specs=(P(("ga", "row", "col"), None, None), P(("ga", "row", "col"), None)),
        check_vma=False,
    )
```

```python
import functools

import jax
import jax.numpy as jnp
from jax import lax
from jax.experimental import pallas as pl
from jax.experimental.pallas import tpu as pltpu
from jax.sharding import PartitionSpec as P

F32 = jnp.float32
BF16 = jnp.bfloat16
NT = (((1,), (1,)), ((), ()))
TN = (((0,), (0,)), ((), ()))


def dot(a, b, dims):
    return lax.dot_general(a, b, dims, preferred_element_type=F32)


def whole(*shape):
    return pl.BlockSpec(shape, lambda *_: (0,) * len(shape))


def in_vmem():
    return pl.BlockSpec(memory_space=pltpu.VMEM)


def pinned(*arrays):
    return [pltpu.with_memory_space_constraint(a, pltpu.VMEM) for a in arrays]


def norm_kernel(pair_ref, gain_ref, shift_ref, out_ref):
    chans = pair_ref.shape[-1]
    pair = pair_ref[...].reshape(-1, chans)
    centred = pair.astype(F32) - dot(pair, jnp.full((chans, chans), 1.0 / chans, BF16), NT)
    spread = jnp.mean(centred * centred, axis=-1, keepdims=True)
    normed = centred * lax.rsqrt(spread + 0.1) * gain_ref[0:1] + shift_ref[0:1]
    rows = pair_ref.shape[0]
    out_ref[pl.ds(pl.program_id(0) * rows, rows)] = normed.astype(BF16).reshape(pair_ref.shape)


def make_norm(pair, gain, shift):
    rows, length, chans = pair.shape
    return pl.pallas_call(
        norm_kernel,
        grid=(rows // 4,),
        in_specs=[
            pl.BlockSpec((4, length, chans), lambda r: (r, 0, 0)),
            whole(*gain.shape),
            whole(*shift.shape),
        ],
        out_specs=in_vmem(),
        out_shape=jax.ShapeDtypeStruct(pair.shape, BF16),
        cost_estimate=pl.CostEstimate(
            flops=rows * length * chans * 100, bytes_accessed=rows * length * chans * 4, transcendentals=0
        ),
        name="norm",
    )(pair, gain, shift)


def weight(mine_ref, other_ref, n):
    mine, other = mine_ref[n], other_ref[n]
    first = lax.axis_index("col") == 0
    return jnp.concatenate([jnp.where(first, mine, other), jnp.where(first, other, mine)], axis=0)


def side_kernel(side, lag, mask_sref, normed_ref, maskk_ref, mine_ref, other_ref, b_ref, out_ref, stage):
    rows, length, chans = normed_ref.shape
    chips, share = out_ref.shape[:2]
    width = stage.shape[1]
    pitch = stage.shape[0] // chips
    core = lax.axis_index("col")
    if lag:
        pl.when(core == 1)(lambda: pl.delay(lag))
    base = (lax.axis_index("row") * lax.axis_size("col") + core) * rows
    bias = jnp.transpose(jnp.concatenate([b_ref[...], jnp.zeros((3, chans), F32)], axis=0))
    w_value = weight(mine_ref, other_ref, 2 * side)
    w_gate = weight(mine_ref, other_ref, 2 * side + 1)
    for k in range(length // width):
        normed = normed_ref[:, k * width : (k + 1) * width, :].reshape(rows * width, chans)
        value = dot(w_value, normed, NT) + bias[:, 2 * side : 2 * side + 1]
        gate = dot(w_gate, normed, NT) + bias[:, 2 * side + 1 : 2 * side + 2]
        value = jax.nn.sigmoid(gate) * value
        mask_k = maskk_ref[:, k * width : (k + 1) * width].astype(F32)
        for r in range(rows):
            part = value[:, r * width : (r + 1) * width] * (mask_k * mask_sref[base + r].astype(F32))
            for c in range(share):
                stage[pl.ds(c * rows + r, chips, stride=pitch), :] = part[c * chips : (c + 1) * chips]
        for z in range(chips):
            block = stage[z * pitch : z * pitch + share * rows, :].reshape(share, rows, width)
            out_ref[z, :, :, k * width : (k + 1) * width] = block.astype(BF16)


def make_side(side, lag, normed, mask, w_mine, w_other, b_in, chips):
    rows, length, chans = normed.shape
    share = chans // chips
    return pl.pallas_call(
        functools.partial(side_kernel, side, lag),
        in_specs=[pl.BlockSpec(memory_space=pltpu.SMEM)] + [in_vmem()] * 5,
        out_specs=in_vmem(),
        out_shape=jax.ShapeDtypeStruct((chips, share, rows, length), BF16),
        scratch_shapes=[pltpu.VMEM((chips * (share * rows + 8), 128), F32)],
        cost_estimate=pl.CostEstimate(
            flops=4 * rows * length * chans * chans, bytes_accessed=rows * length * chans * 4, transcendentals=0
        ),
        name=("left", "right")[side],
    )(mask, normed, mask.reshape(1, length), w_mine, w_other, b_in)


def gate_kernel(normed_ref, mine_ref, other_ref, b_ref, out_ref):
    normed = normed_ref[pl.program_id(0)]
    pre = dot(normed, weight(mine_ref, other_ref, 4), NT) + b_ref[4:5]
    out_ref[0] = jax.nn.sigmoid(pre)


def make_gate(normed, w_mine, w_other, b_in):
    rows, length, chans = normed.shape
    return pl.pallas_call(
        gate_kernel,
        grid=(rows,),
        in_specs=[in_vmem()] * 4,
        out_specs=pl.BlockSpec((1, length, chans), lambda r: (r, 0, 0)),
        out_shape=jax.ShapeDtypeStruct((rows, length, chans), F32),
        cost_estimate=pl.CostEstimate(
            flops=2 * rows * length * chans * chans, bytes_accessed=rows * length * chans * 6, transcendentals=0
        ),
        name="gate",
    )(normed, w_mine, w_other, b_in)


def triangle_kernel(left_ref, right_ref, other_ref, out_ref):
    chips, share, rows, length = left_ref.shape
    half = chips * rows
    core = lax.axis_index("col")
    for c in range(share):
        left = left_ref[:, c].reshape(half, length)
        mine = right_ref[:, c].reshape(half, length)
        other = other_ref[:, c].reshape(half, length)
        first = jnp.where(core == 0, mine, other)
        second = jnp.where(core == 0, other, mine)
        out_ref[:, c, :, 0:half] = dot(left, first, NT).astype(BF16).reshape(chips, rows, half)
        out_ref[:, c, :, half : 2 * half] = dot(left, second, NT).astype(BF16).reshape(chips, rows, half)


def make_triangle(left, right, other):
    return pl.pallas_call(
        triangle_kernel,
        in_specs=[in_vmem()] * 3,
        out_specs=in_vmem(),
        out_shape=jax.ShapeDtypeStruct(left.shape, BF16),
        name="triangle",
    )(*pinned(left), right, *pinned(other))


def finish_kernel(
    prod_ref,
    gate_ref,
    pair_ref,
    w_ref,
    b_ref,
    cols_ref,
    headt_ref,
    headb_ref,
    headbt_ref,
    update_ref,
    send_ref,
    own_ref,
    stage,
    sendst,
):
    chans, rows, _ = prod_ref.shape
    width = stage.shape[2]
    bins = headt_ref.shape[0]
    near = update_ref.shape[1]
    step, steps = pl.program_id(0), pl.num_programs(0)
    gain, shift = cols_ref[:, 0:1], cols_ref[:, 1:2]
    head_t = headt_ref[...]
    head_two = jnp.concatenate([head_t, head_t], axis=0)
    flat = (rows * width, chans)
    logits = []
    for t in range(2):
        at = pl.multiple_of((t * steps + step) * width, width)
        x = prod_ref[:, :, pl.ds(at, width)].astype(F32)
        centred = x - jnp.mean(x, axis=0, keepdims=True)
        spread = jnp.mean(centred * centred, axis=0, keepdims=True)
        stage[t] = (centred * lax.rsqrt(spread + 1.0)).reshape(chans * rows, width)
        normed = [stage[t, pl.ds(r, chans, stride=rows), :] * gain + shift for r in range(rows)]
        normed = jnp.concatenate(normed, axis=1).astype(BF16)
        mixed = dot(normed, w_ref[...], TN) + b_ref[...]
        update = (gate_ref[:, :, t].reshape(flat) * mixed).astype(BF16)
        update_ref[:, :, t] = update.reshape(rows, near, rows, chans)
        pair = pair_ref[:, :, t].reshape(flat)
        new_pair = (pair.astype(F32) + update.astype(F32)).astype(BF16)
        own = dot(head_t, new_pair, NT) + headbt_ref[...]
        for r in range(rows):
            own_ref[t * steps + step, pl.ds(r, bins, stride=rows), :] = own[:, r * width : (r + 1) * width]
        logits.append(dot(new_pair, head_two, NT) + headb_ref[...])
    lane = lax.broadcasted_iota(jnp.int32, logits[0].shape, 1)
    both = jnp.where(lane < bins, logits[0], logits[1])
    for r in range(rows):
        sendst[pl.ds(r, width, stride=rows), :] = both[r * width : (r + 1) * width]
    send_ref[pl.ds(step * near, near)] = sendst[...].reshape(near, rows, rows, 2 * bins).astype(BF16)


def make_finish(prod, gate, pair, w_out, b_out, cols, head_w, head_b):
    chips = prod.shape[0]
    rows, length, chans = pair.shape
    bins = head_w.shape[1]
    cores = 2
    width = 128
    steps = length // (cores * width)
    near = chips // steps
    prod = prod.reshape(chans, rows, length)
    view = (rows, chips, cores, rows, chans)
    wide = pl.BlockSpec((rows, near, cores, rows, chans), lambda z: (0, z, 0, 0, 0))
    head_row = jnp.concatenate([head_b, head_b]).reshape(1, 2 * bins)
    update, send, own = pl.pallas_call(
        finish_kernel,
        grid=(steps,),
        in_specs=[
            in_vmem(),
            wide,
            wide,
            whole(*w_out.shape),
            whole(1, chans),
            whole(*cols.shape),
            whole(bins, chans),
            whole(1, 2 * bins),
            whole(bins, 1),
        ],
        out_specs=[wide, in_vmem(), in_vmem()],
        out_shape=[
            jax.ShapeDtypeStruct(view, BF16),
            jax.ShapeDtypeStruct((chips, rows, rows, 2 * bins), BF16),
            jax.ShapeDtypeStruct((length // width, bins * rows, width), F32),
        ],
        scratch_shapes=[
            pltpu.VMEM((2, chans * rows, width), F32),
            pltpu.VMEM((near * rows * rows, 2 * bins), F32),
        ],
        name="finish",
    )(
        *pinned(prod),
        gate.reshape(view),
        pair.reshape(view),
        w_out,
        b_out.reshape(1, chans),
        cols,
        jnp.transpose(head_w),
        head_row,
        head_b.reshape(bins, 1),
    )
    return update.reshape(rows, length, chans), send, own


def loss_kernel(mask_sref, own_ref, mine_ref, other_ref, targets_ref, maskk_ref, out_ref, stage):
    chips, rows, _, lanes = mine_ref.shape
    bins = lanes // 2
    half = chips * rows
    length = 2 * half
    core = lax.axis_index("col")
    base = (lax.axis_index("row") * lax.axis_size("col") + core) * rows
    pick_row = lax.broadcasted_iota(jnp.int32, (bins, lanes), 0) + core * bins
    pick = jnp.where(pick_row == lax.broadcasted_iota(jnp.int32, (bins, lanes), 1), 1.0, 0.0).astype(BF16)
    for r in range(rows):
        at = pl.ds(r, bins, stride=rows)
        mine = dot(pick, mine_ref[:, r].reshape(half, lanes), NT)
        other = dot(pick, other_ref[:, r].reshape(half, lanes), NT)
        first = jnp.where(core == 0, mine, other)
        second = jnp.where(core == 0, other, mine)
        for q in range(half // 128):
            stage[q, at, :] = first[:, q * 128 : (q + 1) * 128]
            stage[half // 128 + q, at, :] = second[:, q * 128 : (q + 1) * 128]
    symmetric = jnp.concatenate([own_ref[q] + stage[q] for q in range(length // 128)], axis=1)
    symmetric = symmetric.reshape(bins, rows, length)
    top = jnp.max(symmetric, axis=0)
    total = jnp.sum(jnp.exp(symmetric - top[None]), axis=0)
    bin_index = lax.broadcasted_iota(jnp.int32, (bins, rows, length), 0)
    picked = jnp.sum(jnp.where(targets_ref[...][None] == bin_index, symmetric, 0.0), axis=0)
    loss = top + jnp.log(total) - picked
    high = loss.astype(BF16)
    rest = loss - high.astype(F32)
    middle = rest.astype(BF16)
    low = (rest - middle.astype(F32)).astype(BF16)
    spot = lax.broadcasted_iota(jnp.int32, (length, length), 0)
    place = lax.broadcasted_iota(jnp.int32, (length, length), 1)
    come = (place // rows % 2) * half + (place // (2 * rows)) * rows + place % rows
    order = jnp.where(spot == come, 1.0, 0.0).astype(BF16)
    natural = dot(high, order, (((1,), (0,)), ((), ())))
    natural += dot(middle, order, (((1,), (0,)), ((), ())))
    natural += dot(low, order, (((1,), (0,)), ((), ())))
    row = lax.broadcasted_iota(jnp.int32, (rows, length), 0)
    mask_i = jnp.zeros((rows, length), F32)
    for r in range(rows):
        mask_i = jnp.where(row == r, mask_sref[base + r].astype(F32), mask_i)
    out_ref[...] = mask_i * maskk_ref[...].astype(F32) * natural


def make_loss(mask, own, mine, other, targets):
    rows, length = targets.shape
    return pl.pallas_call(
        loss_kernel,
        in_specs=[pl.BlockSpec(memory_space=pltpu.SMEM)] + [in_vmem()] * 5,
        out_specs=in_vmem(),
        out_shape=jax.ShapeDtypeStruct((rows, length), F32),
        scratch_shapes=[pltpu.VMEM(own.shape, F32)],
        name="loss",
    )(mask, own, *pinned(mine, other), targets, mask.reshape(1, length))


LAG_NS = 38000


def local(
    pair, residue_mask, targets, ln_gain, ln_shift, w_in, b_in, w_out, b_out, head_weight, head_bias
):
    rows, length, chans = pair.shape
    chips = lax.axis_size("row")
    share = chans // chips
    swap = functools.partial(lax.ppermute, axis_name="col", perm=[(0, 1), (1, 0)])
    exchange = lambda v: lax.all_to_all(v, "row", split_axis=0, concat_axis=0, tiled=True)
    by_owner = lambda v: jnp.swapaxes(v.reshape(share, chips, -1), 0, 1).reshape(chans, -1)
    w_mine = jnp.transpose(w_in, (0, 2, 1))
    w_other = swap(w_mine)
    out_other = swap(w_out)
    normed = make_norm(pair, ln_gain, ln_shift)
    right = make_side(1, LAG_NS, normed, residue_mask, w_mine, *pinned(w_other), b_in, chips)
    right, out_other = lax.optimization_barrier((right, out_other))
    right = exchange(right)
    left = make_side(0, 0, normed, residue_mask, w_mine, w_other, b_in, chips)
    gate = make_gate(normed, w_mine, w_other, b_in)
    first = lax.axis_index("col") == 0
    w_full = jnp.concatenate([jnp.where(first, w_out, out_other), jnp.where(first, out_other, w_out)], axis=0)
    w_full = by_owner(w_full)
    cols = by_owner(jnp.stack([ln_gain[1], ln_shift[1]], axis=1))
    targets = jnp.swapaxes(targets.reshape(rows, chips, 2, rows), 1, 2).reshape(rows, length)
    left, targets, w_full, cols = lax.optimization_barrier((left, targets, w_full, cols))
    right_other = swap(right)
    left = exchange(left)
    product = exchange(make_triangle(left, right, right_other))
    update, send, own = make_finish(product, gate, pair, w_full, b_out, cols, head_weight, head_bias)
    mine = exchange(send)
    loss = make_loss(residue_mask, own, mine, swap(mine), targets)
    return (update, loss)


def solution(mesh):
    placed = (
        P(("ga", "row", "col"), None, None),
        P("ga"),
        P(("ga", "row", "col"), None),
        P(),
        P(),
        P(None, None, "col"),
        P(),
        P("col", None),
        P(),
        P(),
        P(),
    )
    return jax.shard_map(
        local,
        mesh=mesh,
        in_specs=placed,
        out_specs=(P(("ga", "row", "col"), None, None), P(("ga", "row", "col"), None)),
        check_vma=False,
    )
```
